512 devices in a mesh: row: 16 (over z, core), col: 32 (over x, y).
Axes of the slice: x: 4, y: 8, z: 8, core: 2. Of those that a mesh axis runs over, the one named last changes fastest.
Arguments:
- gram: bfloat16 [2, 16, 384, 1, 32, 384], P(None, 'row', None, None, 'col'), may hold values from -1 to 20, as said below
Outputs:
- swept: float32 [2, 16, 384, 1, 32, 384], P(None, 'row', None, None, 'col')
The draws below stay inside these ranges and needn't reach their ends.
Inputs may be any that keep to these rules, and one draw needn't show every extreme that they name: gram is symmetric and positive definite.
All inputs are finite; a program needn't handle non-finite values.
Results may differ from the reference program's by a relative error of at most 0.0003.
Values sent between devices are 32-bit elements; how exact they have to be, the bound alone decides.
A program may use at most 64 MiB of HBM per device.

```python
import math
import jax
import jax.numpy as jnp
from jax import lax

TB = 384
LC = 1
PANELS = 2
LR = 2
ORDER = 12288
N_ROW = 16
N_COL = 32


def draw_gram(key, part):
    key_noise, key_diagonal = jax.random.split(key, 2)
    noise = jax.random.truncated_normal(key_noise, -4.0, 4.0, (ORDER, ORDER), jnp.float32)
    spread = 1.2 / math.sqrt(2.0 * ORDER)
    symmetric = (noise + noise.T) * spread
    diagonal = jax.random.uniform(key_diagonal, (ORDER,), jnp.float32, 3.0, 6.0)
    matrix = symmetric + jnp.diag(diagonal)
    return matrix.astype(jnp.bfloat16).reshape(LR, N_ROW, TB, LC, N_COL, TB)


def setup_inputs(seed: int = 0) -> dict:
    arg_keys = jax.random.split(jax.random.key(seed), 2)
    gram = draw_gram(jax.random.fold_in(arg_keys[1], 71), 0)
    return {"gram": gram}


def reference(gram):
    matrix = gram.astype(jnp.float32).reshape(ORDER, ORDER)
    identity = jnp.eye(TB, dtype=jnp.float32)
    for number in range(PANELS):
        lower = number * TB
        upper = lower + TB
        factor = jnp.linalg.cholesky(matrix[lower:upper, lower:upper])
        right_side = matrix[lower:upper].at[:, lower:upper].set(identity)
        solved = jax.scipy.linalg.cho_solve((factor, True), right_side)
        shifted = solved.at[:, lower:upper].add(identity)

        def sweep_rows(index, current):
            start = (index * TB).astype(jnp.int32)
            rows = lax.dynamic_slice(current, (start, jnp.int32(0)), (TB, ORDER))
            fresh = rows - jnp.dot(rows[:, lower:upper].astype(jnp.float32), shifted.astype(jnp.float32), precision=lax.Precision.HIGHEST, preferred_element_type=jnp.float32)
            return lax.dynamic_update_slice(current, fresh, (start, jnp.int32(0)))
        matrix = lax.fori_loop(0, ORDER // TB, sweep_rows, matrix)
        matrix = matrix.at[lower:upper].set(solved)
    return matrix.reshape(gram.shape)
```

```python
import functools

import jax
import jax.numpy as jnp
from jax import lax
from jax.experimental import pallas as pl
from jax.experimental.pallas import tpu as pltpu
from jax.sharding import Mesh
from jax.sharding import PartitionSpec as P

F32, BF16 = jnp.float32, jnp.bfloat16
MESH = pl.DeviceIdType.MESH
B = 128
NT = B // 8


def row_all(x, k):
    return jnp.broadcast_to(x[k : k + 1, :], (8, 128))


def row_pick(x, k):
    return jnp.take_along_axis(x, jnp.full((8, 128), k, jnp.int32), axis=0)


def lane_all(x, j):
    return jnp.broadcast_to(x[:, j : j + 1], (8, 128))


def tree(xs):
    xs = list(xs)
    while len(xs) > 1:
        xs = [sum(xs[i : i + 2][1:], xs[i]) for i in range(0, len(xs), 2)]
    return xs[0]


def inverse8(cols, sub):
    cols = list(cols)
    pivot = row_pick(cols[0], 0)
    for k in range(8):
        q = 1.0 / pivot
        if k < 7:
            cross = row_pick(cols[k], k + 1) * row_pick(cols[k + 1], k)
            pivot = row_pick(cols[k + 1], k + 1) - cross * q
        own = sub == k
        cq = cols[k] * q
        new = []
        for j in range(8):
            if j == k:
                new.append(jnp.where(own, q, -cq))
            else:
                r = row_pick(cols[j], k)
                new.append(jnp.where(own, r * q, cols[j] - cq * r))
        cols = new
    return cols


def inverse128(tiles):
    lane = lax.broadcasted_iota(jnp.int32, (8, 128), 1)
    sub = lax.broadcasted_iota(jnp.int32, (8, 128), 0)
    a = list(tiles)
    for s in range(NT):
        inv = inverse8([lane_all(a[s], 8 * s + j) for j in range(8)], sub)
        inside = (lane >= 8 * s) & (lane < 8 * s + 8)
        r = jnp.where(inside, jnp.where(lane - 8 * s == sub, 1.0, 0.0), a[s])
        w = tree([inv[k] * row_all(r, k) for k in range(8)])
        wr = [row_all(w, k) for k in range(8)]
        for t in range(NT):
            if t != s:
                acc = tree([lane_all(a[t], 8 * s + k) * wr[k] for k in range(8)])
                a[t] = jnp.where(inside, 0.0, a[t]) - acc
        a[s] = w
    return a


def split(x):
    hi = x.astype(BF16)
    return hi, (x - hi.astype(F32)).astype(BF16)


def dot(a, b):
    return jnp.dot(a, b, preferred_element_type=F32)


def dot3(a, b):
    return dot(a[0], b[0]) + (dot(a[0], b[1]) + dot(a[1], b[0]))


def eliminate(t, n):
    @pl.loop(0, n // B)
    def _(k):
        o = pl.multiple_of(k * B, B)
        tiles = [t[pl.ds(pl.multiple_of(o + 8 * i, 8), 8), pl.ds(o, B)] for i in range(NT)]
        inv = jnp.concatenate(inverse128(tiles), axis=0)
        for kk in range(n // B):

            @pl.when(k == kk)
            def _():
                own = slice(kk * B, kk * B + B)
                w = dot3(split(inv), split(t[own, kk * B + B :]))
                ws = split(w)
                for i in range(n // B):
                    if i != kk:
                        rows = slice(i * B, i * B + B)
                        t[rows, kk * B + B :] = t[rows, kk * B + B :] - dot3(split(t[rows, own]), ws)
                t[own, kk * B + B :] = w


def kernel(
    nz, nx, ny, tb, g_ref, out_ref, gf, cb, ob, t, sb,
    rc, ro, rg, rs, s_scat, s_y, s_x, s_xf, s_o, s_g, s_z, s_s,
):
    z, core, x, y = (lax.axis_index(a) for a in ("z", "core", "x", "y"))
    mate = 1 - core
    quarter = tb // nx
    step = quarter // 2
    s_step = tb // 4
    in_panel = (x == 0) & (y < 2)
    on_top = z == 0
    pending = []

    def put(cond, src, dst, send, recv, to):
        copy = pltpu.make_async_remote_copy(
            src_ref=src, dst_ref=dst, send_sem=send, recv_sem=recv, device_id=to, device_id_type=MESH
        )
        if cond is None:
            copy.start()
        else:
            pl.when(cond)(copy.start)
        pending.append((cond, copy))

    def arrived(cond, ref, recv):
        copy = pltpu.make_async_remote_copy(
            src_ref=ref, dst_ref=ref, send_sem=s_g, recv_sem=recv, device_id={"core": mate}, device_id_type=MESH
        )
        if cond is None:
            copy.wait_recv()
        else:
            pl.when(cond)(copy.wait_recv)

    def near(i, n):
        return lax.rem(i + n, n)

    for h in range(2):
        gf[h] = g_ref[h].astype(F32)
    for p in range(2):

        @pl.when((x == 0) & (y == p))
        def _():
            for h in range(2):
                cb[h, p, 0:quarter, :] = g_ref[h, 0:quarter, :].astype(F32)

    barrier = pltpu.get_barrier_semaphore()
    peers = [{"x": near(x + i, nx)} for i in range(1, nx)]
    peers += [{"y": near(y + 1, ny)}, {"y": near(y - 1, ny)}]
    peers += [{"z": near(z + 1, nz)}, {"z": near(z - 1, nz)}, {"core": mate}]
    for peer in peers:
        pl.semaphore_signal(barrier, inc=1, device_id=peer, device_id_type=MESH)
    pl.semaphore_wait(barrier, len(peers))

    put(on_top, gf.at[0], ob.at[2], s_g, rg, {"core": mate})

    def rows(q, k):
        return pl.ds(pl.multiple_of(q * quarter + k * step, 8), step)

    def to_mate(p, q, k):
        ref = cb.at[0, p, rows(q, k), :]
        put(on_top, ref, ob.at[p, rows(q, k), :], s_o.at[p, q, k], ro.at[p, q, k], {"core": mate})

    def also(gate, cond):
        return cond if gate is None else gate if cond is None else gate & cond

    def scatter(h, gate=None):
        for p in range(2):
            for k in range(2):
                for q in range(1, nx):
                    put(
                        also(gate, (x == 0) & (y == p)), gf.at[h, rows(q, k), :], cb.at[h, p, rows(q, k), :],
                        s_scat.at[h, p, k, q - 1], rc.at[h, p, q, k], {"x": q},
                    )

    def spread(h, gate=None):
        for k in range(2):
            for p in range(2):
                far = near(y - p, ny)
                ref = cb.at[h, p, rows(x, k), :]
                sem = rc.at[h, p, x, k]
                arrived(also(gate, (x > 0) | (y != p)), ref, sem)
                put(also(gate, far < ny // 2), ref, ref, s_y.at[h, p, k, 0], sem, {"y": near(y + 1, ny)})
                put(also(gate, (far == 0) | (far > ny // 2 + 1)), ref, ref, s_y.at[h, p, k, 1], sem, {"y": near(y - 1, ny)})
                put(gate, ref, ref, s_x.at[h, p, k, 0], sem, {"x": near(x + 1, nx)})
                put(gate, ref, ref, s_x.at[h, p, k, 1], sem, {"x": near(x - 1, nx)})
                if h == 0:
                    to_mate(p, x, k)
        for k in range(2):
            for p in range(2):
                for side in (-1, 1):
                    q = near(x + side, nx)
                    ref = cb.at[h, p, rows(q, k), :]
                    arrived(gate, ref, rc.at[h, p, q, k])
                    if side == (-1, 1)[p]:
                        put(gate, ref, ref, s_xf.at[h, p, k], rc.at[h, p, q, k], {"x": near(x - side, nx)})
                    if h == 0:
                        to_mate(p, q, k)
        for k in range(2):
            for p in range(2):
                q = near(x + 2, nx)
                arrived(gate, cb.at[h, p, rows(q, k), :], rc.at[h, p, q, k])
                if h == 0:
                    to_mate(p, q, k)

    scatter(0)
    spread(0)

    @pl.when(on_top)
    def _():
        arrived(None, ob.at[2], rg)
        for p in range(2):
            for q in range(nx):
                for k in range(2):
                    arrived(None, ob.at[p, rows(q, k), :], ro.at[p, q, k])
        r0 = lax.broadcasted_iota(jnp.int32, (tb, tb), 0)
        r1 = lax.broadcasted_iota(jnp.int32, (tb, tb), 1)
        eye = jnp.where(r0 == r1, 1.0, 0.0).astype(F32)
        mine = pl.ds(pl.multiple_of(core * tb, tb), tb)
        other = pl.ds(pl.multiple_of(mate * tb, tb), tb)
        for p in range(2):
            t[mine, p * tb : p * tb + tb] = cb[0, p]
            t[other, p * tb : p * tb + tb] = ob[p]
        t[mine, 2 * tb :] = jnp.where(in_panel, jnp.where(y == core, eye, 0.0), gf[0])
        t[other, 2 * tb :] = jnp.where(in_panel, jnp.where(y == mate, eye, 0.0), ob[2])
        eliminate(t, 2 * tb)
        for p in range(2):
            sb[p] = t[p * tb : p * tb + tb, 2 * tb :]

    scatter(1, z > 0)
    spread(1, z > 0)

    def s_rows(k):
        return pl.ds(k * s_step, s_step)

    for k in range(4):
        ref = sb.at[core, s_rows(k), :]
        sem = rs.at[core, k]
        arrived(z > 0, ref, sem)
        put(z < nz // 2, ref, ref, s_z.at[k, 0], sem, {"z": near(z + 1, nz)})
        put((z == 0) | (z > nz // 2 + 1), ref, ref, s_z.at[k, 1], sem, {"z": near(z - 1, nz)})
        put(z > 0, ref, ref, s_s.at[k], sem, {"core": mate})
    scatter(1, on_top)
    spread(1, on_top)
    for k in range(4):
        arrived(z > 0, sb.at[mate, s_rows(k), :], rs.at[mate, k])

    ss = [split(sb[p]) for p in range(2)]
    for h in range(2):
        total = jnp.where(in_panel, 0.0, gf[h])
        for p in range(2):
            c = cb[h, p].astype(BF16)
            total = total - (dot(c, ss[p][0]) + dot(c, ss[p][1]))
        out_ref[h] = total

    @pl.when(on_top)
    def _():
        out_ref[0] = sb[core]

    for cond, copy in pending:
        if cond is None:
            copy.wait_send()
        else:
            pl.when(cond)(copy.wait_send)


def on_device(nz, nx, ny, gram):
    tb = gram.shape[2]
    block = gram.reshape(2, tb, tb)
    dma = pltpu.SemaphoreType.DMA
    out = pl.pallas_call(
        functools.partial(kernel, nz, nx, ny, tb),
        out_shape=jax.ShapeDtypeStruct((2, tb, tb), F32),
        in_specs=[pl.BlockSpec(memory_space=pltpu.VMEM)],
        out_specs=pl.BlockSpec(memory_space=pltpu.VMEM),
        scratch_shapes=[
            pltpu.VMEM((2, tb, tb), F32),
            pltpu.VMEM((2, 2, tb, tb), F32),
            pltpu.VMEM((3, tb, tb), F32),
            pltpu.VMEM((2 * tb, 3 * tb), F32),
            pltpu.VMEM((2, tb, tb), F32),
            dma((2, 2, nx, 2)),
            dma((2, nx, 2)),
            dma(()),
            dma((2, 4)),
            dma((2, 2, 2, nx - 1)),
            dma((2, 2, 2, 2)),
            dma((2, 2, 2, 2)),
            dma((2, 2, 2)),
            dma((2, nx, 2)),
            dma(()),
            dma((4, 2)),
            dma((4,)),
        ],
        compiler_params=pltpu.CompilerParams(
            collective_id=0, has_side_effects=True, vmem_limit_bytes=48 << 20
        ),
    )(block)
    return out.reshape(gram.shape)


def solution(mesh):
    shape = (8, 2, 4, 8)
    torus = Mesh(mesh.devices.reshape(shape), ("z", "core", "x", "y"))
    spec = P(None, ("z", "core"), None, None, ("x", "y"), None)
    return jax.shard_map(
        functools.partial(on_device, shape[0], shape[2], shape[3]),
        mesh=torus,
        in_specs=(spec,),
        out_specs=spec,
        check_vma=False,
    )
```

```python
import functools

import jax
import jax.numpy as jnp
from jax import lax
from jax.experimental import pallas as pl
from jax.experimental.pallas import tpu as pltpu
from jax.sharding import Mesh
from jax.sharding import PartitionSpec as P

F32, BF16 = jnp.float32, jnp.bfloat16
MESH = pl.DeviceIdType.MESH
B = 128
NT = B // 8


def row_all(x, k):
    return jnp.broadcast_to(x[k : k + 1, :], (8, 128))


def row_pick(x, k):
    return jnp.take_along_axis(x, jnp.full((8, 128), k, jnp.int32), axis=0)


def lane_all(x, j):
    return jnp.broadcast_to(x[:, j : j + 1], (8, 128))


def tree(xs):
    xs = list(xs)
    while len(xs) > 1:
        xs = [sum(xs[i : i + 2][1:], xs[i]) for i in range(0, len(xs), 2)]
    return xs[0]


def inverse8(cols, sub):
    cols = list(cols)
    pivot = row_pick(cols[0], 0)
    for k in range(8):
        q = 1.0 / pivot
        if k < 7:
            cross = row_pick(cols[k], k + 1) * row_pick(cols[k + 1], k)
            pivot = row_pick(cols[k + 1], k + 1) - cross * q
        own = sub == k
        cq = cols[k] * q
        new = []
        for j in range(8):
            if j == k:
                new.append(jnp.where(own, q, -cq))
            else:
                r = row_pick(cols[j], k)
                new.append(jnp.where(own, r * q, cols[j] - cq * r))
        cols = new
    return cols


def inverse128(tiles):
    lane = lax.broadcasted_iota(jnp.int32, (8, 128), 1)
    sub = lax.broadcasted_iota(jnp.int32, (8, 128), 0)
    a = list(tiles)
    for s in range(NT):
        inv = inverse8([lane_all(a[s], 8 * s + j) for j in range(8)], sub)
        inside = (lane >= 8 * s) & (lane < 8 * s + 8)
        r = jnp.where(inside, jnp.where(lane - 8 * s == sub, 1.0, 0.0), a[s])
        w = tree([inv[k] * row_all(r, k) for k in range(8)])
        wr = [row_all(w, k) for k in range(8)]
        for t in range(NT):
            if t != s:
                acc = tree([lane_all(a[t], 8 * s + k) * wr[k] for k in range(8)])
                a[t] = jnp.where(inside, 0.0, a[t]) - acc
        a[s] = w
    return a


def split(x):
    hi = x.astype(BF16)
    return hi, (x - hi.astype(F32)).astype(BF16)


def dot(a, b):
    return jnp.dot(a, b, preferred_element_type=F32)


def dot3(a, b):
    return dot(a[0], b[0]) + (dot(a[0], b[1]) + dot(a[1], b[0]))


def dot3_t(a, b):
    t = lambda u, v: lax.dot_general(u, v, (((1,), (1,)), ((), ())), preferred_element_type=F32)
    return t(a[0], b[0]) + (t(a[0], b[1]) + t(a[1], b[0]))


NB = 6
HALF = 3


def kernel(
    nz, nx, ny, tb, g_ref, out_ref, cb, rb, t11, fb, xs, dv, vb, lh, ll, xh, xl, yh, yl, zh, zl, vh, vl,
    rc, rm, rg, rt, rr, rf, s_scat, s_y, s_x, s_xf, s_m, s_g, s_t, s_rz, s_rm, sf,
):
    z, core, x, y = (lax.axis_index(a) for a in ("z", "core", "x", "y"))
    mate = 1 - core
    is0, is1 = core == 0, core == 1
    quarter = tb // nx
    top = z == 0
    root = is0 & top & (x == 0) & (y == 0)
    in_panel = (x == 0) & (y < 2)
    to_other = {"core": mate}
    pending = []

    def make(src, dst, send, recv, to):
        return pltpu.make_async_remote_copy(
            src_ref=src, dst_ref=dst, send_sem=send, recv_sem=recv, device_id=to, device_id_type=MESH
        )

    def put(cond, src, dst, send, recv, to):
        copy = make(src, dst, send, recv, to)
        pl.when(cond)(copy.start)
        pending.append((cond, copy))

    def arrived(cond, ref, recv):
        pl.when(cond)(make(ref, ref, s_t, recv, to_other).wait_recv)

    def near(i, n):
        return lax.rem(i + n, n)

    def rows(q):
        return pl.ds(pl.multiple_of(q * quarter, 8), quarter)

    for p in range(2):

        @pl.when((x == 0) & (y == p))
        def _():
            for h in range(2):
                cb[core, h, p] = g_ref[h].astype(F32)

    @pl.when(top)
    def _():
        rb[core] = g_ref[0].astype(F32)

    barrier = pltpu.get_barrier_semaphore()
    peers = [{"x": near(x + i, nx)} for i in range(1, nx)]
    for i in (-2, -1, 1, 2):
        peers += [{"y": near(y + i, ny)}, {"z": near(z + i, nz)}]
    peers += [to_other, {"y": y + 1 - 2 * lax.rem(y, 2), "core": mate}]
    for peer in peers:
        pl.semaphore_signal(barrier, inc=1, device_id=peer, device_id_type=MESH)
    pl.semaphore_wait(barrier, len(peers))

    def r_rows(c):
        return pl.ds(c * quarter, quarter)

    for c in range(4):
        ref = rb.at[1, r_rows(c), :]
        put(top & is1, ref, ref, s_rm.at[1, c], rr.at[1, c], to_other)
    put(is1 & top & (x == 0) & (y == 1), cb.at[1, 0, 1], t11, s_t, rt, {"core": 0, "y": 0})

    def needed(h):
        return z > 0 if h == 0 else z >= 0

    for h in range(2):
        for p in range(2):
            ref = cb.at[0, h, p]
            put(is0 & (x == 0) & (y == p) & needed(h), ref, ref, s_g.at[h], rg.at[h], to_other)

    def tree8(i, gate, late):
        hub = gate & ((i == 0) | (i == 2) | (i == 6))
        return [
            (hub, jnp.where(i == 0, 2, i - 1)),
            (hub, jnp.where(i == 0, 6, lax.rem(i + 1, 8))),
            (gate & (i == (2 if late else 3)), 4),
        ]

    for tile in range(2):
        for c in range(4):
            ref = rb.at[tile, r_rows(c), :]
            sem = rr.at[tile, c]
            arrived(is0 if tile else is0 & (z > 0), ref, sem)
            for n, (cond, to) in enumerate(tree8(z, is0, False)):
                put(cond, ref, ref, s_rz.at[tile, c, n], sem, {"z": to})
            put(is0 & (z > 0) if tile else is0, ref, ref, s_rm.at[tile, c] if tile == 0 else s_rz.at[tile, c, 3], sem, to_other)

    def scatter(r, h):
        for p in range(2):
            here = is1 & (x == 0) & (y == p) & needed(h)
            if r == 0:
                arrived(here, cb.at[0, h, p], rg.at[h])
            for q in range(1, nx):
                ref = cb.at[r, h, p, rows(q), :]
                put(here, ref, ref, s_scat.at[r, h, q - 1], rc.at[r, h, p, q], {"x": q})

    def to_mate(gate, r, h, p, q):
        if r == 0:
            ref = cb.at[0, h, p, rows(q), :]
            put(gate, ref, ref, s_m.at[h, p, q], rm.at[h, p, q], to_other)

    def spread(r, h):
        for p in range(2):
            gate = is1 & needed(h)
            src = (x == 0) & (y == p)
            far = near(y - p, ny)
            ref, sem = cb.at[r, h, p, rows(x), :], rc.at[r, h, p, x]
            arrived(gate & ((x > 0) | (y != p)), ref, sem)
            put(gate & (far < ny // 2), ref, ref, s_y.at[r, h, p, 0], sem, {"y": near(y + 1, ny)})
            put(gate & ((far == 0) | (far > ny // 2 + 1)), ref, ref, s_y.at[r, h, p, 1], sem, {"y": near(y - 1, ny)})
            for n, side in enumerate((1, -1)):
                to = near(x + side, nx)
                put(gate & ((to > 0) | (y != p)), ref, ref, s_x.at[r, h, p, n], sem, {"x": to})
            to_mate(gate & ((x > 0) | (y != p)), r, h, p, x)

    def gather(r, h):
        for p in range(2):
            gate = is1 & needed(h)
            get = gate & ((x > 0) | (y != p))
            for side in (-1, 1):
                q = near(x + side, nx)
                ref, sem = cb.at[r, h, p, rows(q), :], rc.at[r, h, p, q]
                arrived(get, ref, sem)
                if side == (-1, 1)[p]:
                    to = near(x - side, nx)
                    put(gate & ((to > 0) | (y != p)), ref, ref, s_xf.at[r, h, p], sem, {"x": to})
                to_mate(get, r, h, p, q)
        for p in range(2):
            get = is1 & needed(h) & ((x > 0) | (y != p))
            q = near(x + 2, nx)
            arrived(get, cb.at[r, h, p, rows(q), :], rc.at[r, h, p, q])
            to_mate(get, r, h, p, q)

    order = [(1, 0), (1, 1), (0, 0), (0, 1)]
    for r, h in order:
        scatter(r, h)
    for n, (r, h) in enumerate(order):
        spread(r, h)
        if n:
            gather(*order[n - 1])
    gather(*order[-1])

    items = [(k, i) for k in range(NB) for i in range(k, NB)]

    def item_sends(k, i):
        late = k >= NB - 2
        on_x = is0 & top & (y == 0)
        ways = [(on_x & (x == 0), {"x": 1}), (on_x & (x == 0), {"x": 3})]
        ways += [(on_x & (x == (0 if late else 1)), {"x": 2})]
        ways += [(c, {"y": to}) for c, to in tree8(y, is0 & top, late)]
        ways += [(c, {"z": to}) for c, to in tree8(z, is0, late)]
        ways += [(is0, to_other)]
        ref = fb.at[k, i]
        return [(c, make(ref, ref, sf.at[k, i, n], rf.at[k, i], to)) for n, (c, to) in enumerate(ways)]

    def relay(gate, k, i):
        @pl.when(gate)
        def _():
            make(fb.at[k, i], fb.at[k, i], s_t, rf.at[k, i], to_other).wait_recv()
            for cond, copy in item_sends(k, i):
                pl.when(cond)(copy.start)

    @pl.when(root)
    def _():
        @pl.loop(0, NB)
        def _(j):
            for jj in range(NB):

                @pl.when(j == jj)
                def _():
                    lo = jj * B
                    if jj == HALF:
                        make(t11, t11, s_t, rt, to_other).wait_recv()
                    acc = 0.0
                    if jj:
                        acc = dot3_t((lh[lo:, :lo], ll[lo:, :lo]), (xh[lo : lo + B, :lo], xl[lo : lo + B, :lo]))
                    if jj < HALF:
                        a = jnp.concatenate([rb[0, lo:, lo : lo + B], rb[1, :, lo : lo + B]], axis=0)
                    else:
                        a = t11[lo - tb :, lo - tb : lo - tb + B]
                    xs[lo:, :] = a - acc

            o = pl.multiple_of(j * B, B)
            tiles = [xs[pl.ds(pl.multiple_of(o + 8 * i, 8), 8), :] for i in range(NT)]
            inv = inverse128(tiles)
            for i in range(NT):
                dv[8 * i : 8 * i + 8, :] = inv[i]
            for jj in range(NB):

                @pl.when(j == jj)
                def _():
                    lo = jj * B
                    fb[jj, jj] = dv[...]
                    if jj < NB - 1:
                        xc = split(xs[lo + B :, :])
                        w = dot3(xc, split(dv[...]))
                        wc = split(w)
                        xh[lo + B :, lo : lo + B], xl[lo + B :, lo : lo + B] = xc
                        lh[lo + B :, lo : lo + B], ll[lo + B :, lo : lo + B] = wc
                        for i in range(jj + 1, NB):
                            fb[jj, i] = w[(i - jj - 1) * B : (i - jj) * B, :]
                    for i in range(jj, NB):
                        for cond, copy in item_sends(jj, i):
                            pl.when(cond)(copy.start)

    others = is0 & jnp.logical_not(root)
    hub = (z == 0) | (z == 2) | (z == 6)
    for k, i in items[:-1]:
        relay(others, k, i)
    relay(others & hub, *items[-1])

    for tile in range(2):
        for c in range(4):
            arrived(is1 & (z > 0) if tile else is1, rb.at[tile, r_rows(c), :], rr.at[tile, c])
    for h in range(2):
        for p in range(2):
            for q in range(nx):
                get = is0 & needed(h) & ((x > 0) | (y != p))
                arrived(get, cb.at[0, h, p, rows(q), :], rm.at[h, p, q])
    for k, i in items[:-1]:
        arrived(is1, fb.at[k, i], rf.at[k, i])

    def unit(shape, shift):
        r = lax.broadcasted_iota(jnp.int32, shape, 0)
        return jnp.where(r - lax.broadcasted_iota(jnp.int32, shape, 1) == shift, 1.0, 0.0).astype(F32)

    def update(lo, hi, first):
        for h in range(2):
            o = h * tb
            c = (vh[o : o + tb, lo:hi], vl[o : o + tb, lo:hi])
            w = (zh[lo:hi, :], zl[lo:hi, :])
            if first:
                keep = jnp.logical_not(in_panel | (top & (h == 0)))
                base = jnp.where(keep, g_ref[h].astype(F32), 0.0)
            else:
                base = out_ref[h]
            out_ref[h] = base - dot3(c, w)

    def solve(k):
        lo = k * B
        w = split(dot3(split(fb[k, k]), (yh[lo : lo + B, :], yl[lo : lo + B, :])))
        zh[lo : lo + B, :], zl[lo : lo + B, :] = w

    for k in range(NB):
        lo = k * B
        for j in range(k):
            lh[lo : lo + B, j * B : j * B + B], ll[lo : lo + B, j * B : j * B + B] = split(fb[j, k])
        p, off = k // HALF, k % HALF * B
        yk = jnp.where(in_panel, jnp.where(y == p, unit((B, tb), -off), 0.0), rb[p, off : off + B, :])
        if k:
            lk = (lh[lo : lo + B, :lo], ll[lo : lo + B, :lo])
            yk = yk - dot3(lk, (yh[:lo, :], yl[:lo, :]))
        yh[lo : lo + B, :], yl[lo : lo + B, :] = split(yk)
        for h in range(2):
            o = h * tb
            if h == 0:

                @pl.when(top)
                def _():
                    vb[...] = jnp.where(core == p, -unit((tb, B), off), 0.0)

                @pl.when(z > 0)
                def _():
                    vb[...] = cb[core, 0, p, :, off : off + B]

            vk = vb[...] if h == 0 else cb[core, h, p, :, off : off + B]
            if k:
                vk = vk - dot3_t((vh[o : o + tb, :lo], vl[o : o + tb, :lo]), lk)
            vh[o : o + tb, lo : lo + B], vl[o : o + tb, lo : lo + B] = split(vk)
        if k < NB - 1:
            solve(k)
    update(0, (NB - 1) * B, True)

    relay(others & jnp.logical_not(hub), *items[-1])
    arrived(is1, fb.at[items[-1][0], items[-1][1]], rf.at[items[-1][0], items[-1][1]])
    solve(NB - 1)
    update((NB - 1) * B, NB * B, False)

    for cond, copy in pending:
        pl.when(cond)(copy.wait_send)
    for k, i in items:
        for cond, copy in item_sends(k, i):
            pl.when(cond)(copy.wait_send)


def on_device(nz, nx, ny, gram):
    tb = gram.shape[2]
    block = gram.reshape(2, tb, tb)
    dma = pltpu.SemaphoreType.DMA
    n = 2 * tb
    wide = [pltpu.VMEM((n, n), BF16)]
    tall = [pltpu.VMEM((n, tb), BF16)]
    out = pl.pallas_call(
        functools.partial(kernel, nz, nx, ny, tb),
        out_shape=jax.ShapeDtypeStruct((2, tb, tb), F32),
        in_specs=[pl.BlockSpec(memory_space=pltpu.VMEM)],
        out_specs=pl.BlockSpec(memory_space=pltpu.VMEM),
        scratch_shapes=[
            pltpu.VMEM((2, 2, 2, tb, tb), F32),
            pltpu.VMEM((2, tb, tb), F32),
            pltpu.VMEM((tb, tb), F32),
            pltpu.VMEM((NB, NB, B, B), F32),
            pltpu.VMEM((n, B), F32),
            pltpu.VMEM((B, B), F32),
            pltpu.VMEM((tb, B), F32),
        ]
        + wide * 4 + tall * 4 + wide * 2
        + [
            dma((2, 2, 2, nx)),
            dma((2, 2, nx)),
            dma((2,)),
            dma(()),
            dma((2, 4)),
            dma((NB, NB)),
            dma((2, 2, nx - 1)),
            dma((2, 2, 2, 2)),
            dma((2, 2, 2, 2)),
            dma((2, 2, 2)),
            dma((2, 2, nx)),
            dma((2,)),
            dma(()),
            dma((2, 4, 4)),
            dma((2, 4)),
            dma((NB, NB, 10)),
        ],
        compiler_params=pltpu.CompilerParams(
            collective_id=0, has_side_effects=True, vmem_limit_bytes=48 << 20
        ),
    )(block)
    return out.reshape(gram.shape)


def solution(mesh):
    shape = (8, 2, 4, 8)
    torus = Mesh(mesh.devices.reshape(shape), ("z", "core", "x", "y"))
    spec = P(None, ("z", "core"), None, None, ("x", "y"), None)
    return jax.shard_map(
        functools.partial(on_device, shape[0], shape[2], shape[3]),
        mesh=torus,
        in_specs=(spec,),
        out_specs=spec,
        check_vma=False,
    )
```

```python
import functools

import jax
import jax.numpy as jnp
from jax import lax
from jax.experimental import pallas as pl
from jax.experimental.pallas import tpu as pltpu
from jax.sharding import Mesh
from jax.sharding import PartitionSpec as P

F32, BF16 = jnp.float32, jnp.bfloat16
MESH = pl.DeviceIdType.MESH
B = 128
NT = B // 8


def row_all(x, k):
    return jnp.broadcast_to(x[k : k + 1, :], (8, 128))


def row_pick(x, k):
    return jnp.take_along_axis(x, jnp.full((8, 128), k, jnp.int32), axis=0)


def lane_all(x, j):
    return jnp.broadcast_to(x[:, j : j + 1], (8, 128))


def tree(xs):
    xs = list(xs)
    while len(xs) > 1:
        xs = [sum(xs[i : i + 2][1:], xs[i]) for i in range(0, len(xs), 2)]
    return xs[0]


def inverse8(cols, sub):
    cols = list(cols)
    pivot = row_pick(cols[0], 0)
    for k in range(8):
        q = 1.0 / pivot
        if k < 7:
            cross = row_pick(cols[k], k + 1) * row_pick(cols[k + 1], k)
            pivot = row_pick(cols[k + 1], k + 1) - cross * q
        own = sub == k
        cq = cols[k] * q
        new = []
        for j in range(8):
            if j == k:
                new.append(jnp.where(own, q, -cq))
            else:
                r = row_pick(cols[j], k)
                new.append(jnp.where(own, r * q, cols[j] - cq * r))
        cols = new
    return cols


def inverse128(tiles):
    lane = lax.broadcasted_iota(jnp.int32, (8, 128), 1)
    sub = lax.broadcasted_iota(jnp.int32, (8, 128), 0)
    a = list(tiles)
    for s in range(NT):
        inv = inverse8([lane_all(a[s], 8 * s + j) for j in range(8)], sub)
        inside = (lane >= 8 * s) & (lane < 8 * s + 8)
        r = jnp.where(inside, jnp.where(lane - 8 * s == sub, 1.0, 0.0), a[s])
        w = tree([inv[k] * row_all(r, k) for k in range(8)])
        wr = [row_all(w, k) for k in range(8)]
        for t in range(NT):
            if t != s:
                acc = tree([lane_all(a[t], 8 * s + k) * wr[k] for k in range(8)])
                a[t] = jnp.where(inside, 0.0, a[t]) - acc
        a[s] = w
    return a


def split(x):
    hi = x.astype(BF16)
    return hi, (x - hi.astype(F32)).astype(BF16)


def dot(a, b):
    return jnp.dot(a, b, preferred_element_type=F32)


def dot3(a, b):
    return dot(a[0], b[0]) + (dot(a[0], b[1]) + dot(a[1], b[0]))


def dot3_t(a, b):
    t = lambda u, v: lax.dot_general(u, v, (((1,), (1,)), ((), ())), preferred_element_type=F32)
    return t(a[0], b[0]) + (t(a[0], b[1]) + t(a[1], b[0]))


NB = 6
HALF = 3
CUT = 1
SPAN = 1


def kernel(
    nz, nx, ny, tb, g_ref, out_ref, cb, rb, t11, fb, xs, dv, vb, lh, ll, xh, xl, yh, yl, zh, zl, vh, vl,
    rc, rm, rg, rt, rr, rf, s_scat, s_y, s_x, s_xf, s_m, s_g, s_t, s_r, sf,
):
    z, core, x, y = (lax.axis_index(a) for a in ("z", "core", "x", "y"))
    mate = 1 - core
    is0, is1 = core == 0, core == 1
    quarter = tb // nx
    top = z == 0
    root = is0 & top & (x == 0) & (y == 0)
    in_panel = (x == 0) & (y < 2)
    to_other = {"core": mate}
    pending = []

    def make(src, dst, send, recv, to):
        return pltpu.make_async_remote_copy(
            src_ref=src, dst_ref=dst, send_sem=send, recv_sem=recv, device_id=to, device_id_type=MESH
        )

    def put(cond, src, dst, send, recv, to):
        copy = make(src, dst, send, recv, to)
        pl.when(cond)(copy.start)
        pending.append((cond, copy))

    def arrived(cond, ref, recv):
        pl.when(cond)(make(ref, ref, s_t, recv, to_other).wait_recv)

    def near(i, n):
        return lax.rem(i + n, n)

    piece = quarter // CUT

    def rows(q, k):
        return pl.ds(pl.multiple_of(q * quarter + k * piece, 8), piece)

    for p in range(2):

        @pl.when((x == 0) & (y == p))
        def _():
            for h in range(2):
                cb[core, h, p] = g_ref[h].astype(F32)

    @pl.when(top)
    def _():
        rb[core] = g_ref[0].astype(F32)

    barrier = pltpu.get_barrier_semaphore()
    peers = [{"x": near(x + i, nx)} for i in range(1, nx)]
    for i in (-2, -1, 1, 2):
        peers += [{"y": near(y + i, ny)}, {"z": near(z + i, nz)}]
    peers += [to_other, {"y": y + 1 - 2 * lax.rem(y, 2), "core": mate}]
    for peer in peers:
        pl.semaphore_signal(barrier, inc=1, device_id=peer, device_id_type=MESH)
    pl.semaphore_wait(barrier, len(peers))

    def tree8(i, gate, last):
        hub = gate & ((i == 0) | (i == 2) | (i == 6))
        return [
            (hub, jnp.where(i == 0, 2, i - 1)),
            (hub, jnp.where(i == 0, 6, lax.rem(i + 1, 8))),
            (gate & last, 4),
        ]

    def r_rows(c):
        return pl.ds(c * quarter, quarter)

    def r_sends(c):
        ref, sem = rb.at[core, r_rows(c), :], rr.at[core, c]
        ways = [(cond, {"z": to}) for cond, to in tree8(z, z >= 0, (is0 & (z == 2)) | (is1 & (z == 6)))]
        ways += [(z >= 0, to_other)]
        return [(cond, make(ref, ref, s_r.at[c, n], sem, to)) for n, (cond, to) in enumerate(ways)]

    def r_relay(gate):
        @pl.when(gate)
        def _():
            for c in range(4):
                ref = rb.at[core, r_rows(c), :]
                pl.when(z > 0)(make(ref, ref, s_t, rr.at[core, c], to_other).wait_recv)
                for cond, copy in r_sends(c):
                    pl.when(cond)(copy.start)

    put(is1 & top & (x == 0) & (y == 1), cb.at[1, 0, 1], t11, s_t, rt, {"core": 0, "y": 0})
    for p in range(2):
        ref = cb.at[0, 1, p]
        put(is0 & top & (x == 0) & (y == p), ref, ref, s_g, rg, to_other)
    r_relay(top)

    busy = (z > 0) | is1

    def part(n):
        return jnp.where(top, 1 - n, core), jnp.where(top, 1, n)

    def scatter(n):
        r, h = part(n)
        for p in range(2):
            here = busy & (x == 0) & (y == p)
            if n:
                arrived(here & top, cb.at[0, 1, p], rg)
            for k in range(CUT):
                for q in (2, 1, 3):
                    ref = cb.at[r, h, p, rows(q, k), :]
                    put(here, ref, ref, s_scat.at[n, q - 1, k], rc.at[n, p, q, k], {"x": q})

    def to_mate(gate, n, p, q, k):
        if n:
            ref = cb.at[0, 1, p, rows(q, k), :]
            put(gate & top, ref, ref, s_m.at[p, q, k], rm.at[p, q, k], to_other)

    def spread(n):
        r, h = part(n)
        for k in range(CUT):
            for p in range(2):
                get = busy & ((x > 0) | (y != p))
                far = near(y - p, ny)
                ref, sem = cb.at[r, h, p, rows(x, k), :], rc.at[n, p, x, k]
                arrived(get, ref, sem)
                put(busy & (far < ny // 2), ref, ref, s_y.at[n, p, k, 0], sem, {"y": near(y + 1, ny)})
                back = busy & ((far == 0) | (far > ny // 2 + 1))
                put(back, ref, ref, s_y.at[n, p, k, 1], sem, {"y": near(y - 1, ny)})
                for i, side in enumerate((1, -1)):
                    to = near(x + side, nx)
                    put(busy & ((to > 0) | (y != p)), ref, ref, s_x.at[n, p, k, i], sem, {"x": to})
                to_mate(get, n, p, x, k)

    def gather(n):
        r, h = part(n)
        for k in range(CUT):
            for p in range(2):
                get = busy & ((x > 0) | (y != p))
                for side in (-1, 1):
                    q = near(x + side, nx)
                    ref, sem = cb.at[r, h, p, rows(q, k), :], rc.at[n, p, q, k]
                    arrived(get, ref, sem)
                    if side == (-1, 1)[p]:
                        to = near(x - side, nx)
                        put(busy & ((to > 0) | (y != p)), ref, ref, s_xf.at[n, p, k], sem, {"x": to})
                    to_mate(get, n, p, q, k)

    def gather_far(n):
        r, h = part(n)
        for k in range(CUT):
            for p in range(2):
                get = busy & ((x > 0) | (y != p))
                q = near(x + 2, nx)
                arrived(get, cb.at[r, h, p, rows(q, k), :], rc.at[n, p, q, k])
                to_mate(get, n, p, q, k)

    scatter(0)
    scatter(1)

    items = [(k, i) for k in range(NB) for i in range(k, NB, SPAN)]

    def blocks(k, i):
        return fb.at[k, i : min(i + SPAN, NB)]

    def item_sends(k, i):
        late = k >= NB - 2
        on_x = is0 & top & (y == 0)
        ways = [(on_x & (x == 0), {"x": 1}), (on_x & (x == 0), {"x": 3})]
        ways += [(on_x & (x == (0 if late else 1)), {"x": 2})]
        ways += [(c, {"y": to}) for c, to in tree8(y, is0 & top, y == (2 if late else 3))]
        ways += [(c, {"z": to}) for c, to in tree8(z, is0, z == (2 if late else 3))]
        ways += [(is0, to_other)]
        ref = blocks(k, i)
        return [(c, make(ref, ref, sf.at[k, i, n], rf.at[k, i], to)) for n, (c, to) in enumerate(ways)]

    def relay(gate, k, i):
        @pl.when(gate)
        def _():
            make(blocks(k, i), blocks(k, i), s_t, rf.at[k, i], to_other).wait_recv()
            for cond, copy in item_sends(k, i):
                pl.when(cond)(copy.start)

    @pl.when(root)
    def _():
        for c in range(4):
            make(rb.at[1, r_rows(c), :], rb.at[1, r_rows(c), :], s_t, rr.at[1, c], to_other).wait_recv()

        @pl.loop(0, NB)
        def _(j):
            for jj in range(NB):

                @pl.when(j == jj)
                def _():
                    lo = jj * B
                    if jj == HALF:
                        make(t11, t11, s_t, rt, to_other).wait_recv()
                    acc = 0.0
                    if jj:
                        acc = dot3_t((lh[lo:, :lo], ll[lo:, :lo]), (xh[lo : lo + B, :lo], xl[lo : lo + B, :lo]))
                    if jj < HALF:
                        a = jnp.concatenate([rb[0, lo:, lo : lo + B], rb[1, :, lo : lo + B]], axis=0)
                    else:
                        a = t11[lo - tb :, lo - tb : lo - tb + B]
                    xs[lo:, :] = a - acc

            o = pl.multiple_of(j * B, B)
            tiles = [xs[pl.ds(pl.multiple_of(o + 8 * i, 8), 8), :] for i in range(NT)]
            inv = inverse128(tiles)
            for i in range(NT):
                dv[8 * i : 8 * i + 8, :] = inv[i]
            for jj in range(NB):

                @pl.when(j == jj)
                def _():
                    lo = jj * B
                    fb[jj, jj] = dv[...]
                    if jj < NB - 1:
                        xc = split(xs[lo + B :, :])
                        w = dot3(xc, split(dv[...]))
                        wc = split(w)
                        xh[lo + B :, lo : lo + B], xl[lo + B :, lo : lo + B] = xc
                        lh[lo + B :, lo : lo + B], ll[lo + B :, lo : lo + B] = wc
                        for i in range(jj + 1, NB):
                            fb[jj, i] = w[(i - jj - 1) * B : (i - jj) * B, :]
                    for i in range(jj, NB, SPAN):
                        for cond, copy in item_sends(jj, i):
                            pl.when(cond)(copy.start)

    others = is0 & jnp.logical_not(root)
    hub = (z == 0) | (z == 2) | (z == 6)

    def step(k):
        for i in range(k, NB, SPAN):
            relay(others, k, i)

    spoke = (z == 2) | (z == 6)
    spread(0)
    r_relay(spoke)
    spread(1)
    step(0)
    gather(0)
    step(1)
    gather(1)
    step(2)
    step(3)
    step(4)
    r_relay(jnp.logical_not(spoke | top))
    relay(others & hub, *items[-1])

    for c in range(4):
        arrived(jnp.logical_not(root), rb.at[mate, r_rows(c), :], rr.at[mate, c])
    for k, i in items[:-1]:
        arrived(is1, blocks(k, i), rf.at[k, i])

    def unit(shape, shift):
        r = lax.broadcasted_iota(jnp.int32, shape, 0)
        return jnp.where(r - lax.broadcasted_iota(jnp.int32, shape, 1) == shift, 1.0, 0.0).astype(F32)

    def update(h, lo, hi, first):
        o = h * tb
        c = (vh[o : o + tb, lo:hi], vl[o : o + tb, lo:hi])
        w = (zh[lo:hi, :], zl[lo:hi, :])
        if first:
            keep = jnp.logical_not(in_panel | (top & (h == 0)))
            base = jnp.where(keep, g_ref[h].astype(F32), 0.0)
        else:
            base = out_ref[h]
        out_ref[h] = base - dot3(c, w)

    def solve(k):
        lo = k * B
        w = split(dot3(split(fb[k, k]), (yh[lo : lo + B, :], yl[lo : lo + B, :])))
        zh[lo : lo + B, :], zl[lo : lo + B, :] = w

    for k in range(NB):
        lo = k * B
        for j in range(k):
            lh[lo : lo + B, j * B : j * B + B], ll[lo : lo + B, j * B : j * B + B] = split(fb[j, k])
        p, off = k // HALF, k % HALF * B
        yk = jnp.where(in_panel, jnp.where(y == p, unit((B, tb), -off), 0.0), rb[p, off : off + B, :])
        if k:
            lk = (lh[lo : lo + B, :lo], ll[lo : lo + B, :lo])
            yk = yk - dot3(lk, (yh[:lo, :], yl[:lo, :]))
        yh[lo : lo + B, :], yl[lo : lo + B, :] = split(yk)
        if k < NB - 1:
            solve(k)

    def columns(h):
        o = h * tb
        for k in range(NB):
            lo = k * B
            p, off = k // HALF, k % HALF * B
            if h == 0:

                @pl.when(top)
                def _():
                    vb[...] = jnp.where(core == p, -unit((tb, B), off), 0.0)

                @pl.when(z > 0)
                def _():
                    vb[...] = cb[core, 0, p, :, off : off + B]

            vk = vb[...] if h == 0 else cb[core, h, p, :, off : off + B]
            if k:
                lk = (lh[lo : lo + B, :lo], ll[lo : lo + B, :lo])
                vk = vk - dot3_t((vh[o : o + tb, :lo], vl[o : o + tb, :lo]), lk)
            vh[o : o + tb, lo : lo + B], vl[o : o + tb, lo : lo + B] = split(vk)
        update(h, 0, (NB - 1) * B, True)

    gather_far(0)
    columns(0)
    gather_far(1)
    for p in range(2):
        for q in range(nx):
            for k in range(CUT):
                get = is0 & top & ((x > 0) | (y != p))
                arrived(get, cb.at[0, 1, p, rows(q, k), :], rm.at[p, q, k])
    columns(1)

    relay(others & jnp.logical_not(hub), *items[-1])
    arrived(is1, blocks(*items[-1]), rf.at[NB - 1, NB - 1])
    solve(NB - 1)
    for h in range(2):
        update(h, (NB - 1) * B, NB * B, False)

    for cond, copy in pending:
        pl.when(cond)(copy.wait_send)
    for copies in [r_sends(c) for c in range(4)] + [item_sends(k, i) for k, i in items]:
        for cond, copy in copies:
            pl.when(cond)(copy.wait_send)


def on_device(nz, nx, ny, gram):
    tb = gram.shape[2]
    block = gram.reshape(2, tb, tb)
    dma = pltpu.SemaphoreType.DMA
    n = 2 * tb
    wide = [pltpu.VMEM((n, n), BF16)]
    tall = [pltpu.VMEM((n, tb), BF16)]
    out = pl.pallas_call(
        functools.partial(kernel, nz, nx, ny, tb),
        out_shape=jax.ShapeDtypeStruct((2, tb, tb), F32),
        in_specs=[pl.BlockSpec(memory_space=pltpu.VMEM)],
        out_specs=pl.BlockSpec(memory_space=pltpu.VMEM),
        scratch_shapes=[
            pltpu.VMEM((2, 2, 2, tb, tb), F32),
            pltpu.VMEM((2, tb, tb), F32),
            pltpu.VMEM((tb, tb), F32),
            pltpu.VMEM((NB, NB, B, B), F32),
            pltpu.VMEM((n, B), F32),
            pltpu.VMEM((B, B), F32),
            pltpu.VMEM((tb, B), F32),
        ]
        + wide * 4 + tall * 4 + wide * 2
        + [
            dma((2, 2, nx, CUT)),
            dma((2, nx, CUT)),
            dma(()),
            dma(()),
            dma((2, 4)),
            dma((NB, NB)),
            dma((2, nx - 1, CUT)),
            dma((2, 2, CUT, 2)),
            dma((2, 2, CUT, 2)),
            dma((2, 2, CUT)),
            dma((2, nx, CUT)),
            dma(()),
            dma(()),
            dma((4, 4)),
            dma((NB, NB, 10)),
        ],
        compiler_params=pltpu.CompilerParams(
            collective_id=0, has_side_effects=True, vmem_limit_bytes=48 << 20
        ),
    )(block)
    return out.reshape(gram.shape)


def solution(mesh):
    shape = (8, 2, 4, 8)
    torus = Mesh(mesh.devices.reshape(shape), ("z", "core", "x", "y"))
    spec = P(None, ("z", "core"), None, None, ("x", "y"), None)
    return jax.shard_map(
        functools.partial(on_device, shape[0], shape[2], shape[3]),
        mesh=torus,
        in_specs=(spec,),
        out_specs=spec,
        check_vma=False,
    )
```

```python
import functools

import jax
import jax.numpy as jnp
from jax import lax
from jax.experimental import pallas as pl
from jax.experimental.pallas import tpu as pltpu
from jax.sharding import Mesh
from jax.sharding import PartitionSpec as P

F32, BF16 = jnp.float32, jnp.bfloat16
MESH = pl.DeviceIdType.MESH
B = 128
NT = B // 8


def row_all(x, k):
    return jnp.broadcast_to(x[k : k + 1, :], (8, 128))


def row_pick(x, k):
    return jnp.take_along_axis(x, jnp.full((8, 128), k, jnp.int32), axis=0)


def lane_all(x, j):
    return jnp.broadcast_to(x[:, j : j + 1], (8, 128))


def tree(xs):
    xs = list(xs)
    while len(xs) > 1:
        xs = [sum(xs[i : i + 2][1:], xs[i]) for i in range(0, len(xs), 2)]
    return xs[0]


def inverse8(cols, sub):
    cols = list(cols)
    pivot = row_pick(cols[0], 0)
    for k in range(8):
        q = 1.0 / pivot
        if k < 7:
            cross = row_pick(cols[k], k + 1) * row_pick(cols[k + 1], k)
            pivot = row_pick(cols[k + 1], k + 1) - cross * q
        own = sub == k
        cq = cols[k] * q
        new = []
        for j in range(8):
            if j == k:
                new.append(jnp.where(own, q, -cq))
            else:
                r = row_pick(cols[j], k)
                new.append(jnp.where(own, r * q, cols[j] - cq * r))
        cols = new
    return cols


def inverse128(tiles):
    lane = lax.broadcasted_iota(jnp.int32, (8, 128), 1)
    sub = lax.broadcasted_iota(jnp.int32, (8, 128), 0)
    a = list(tiles)
    for s in range(NT):
        inv = inverse8([lane_all(a[s], 8 * s + j) for j in range(8)], sub)
        inside = (lane >= 8 * s) & (lane < 8 * s + 8)
        r = jnp.where(inside, jnp.where(lane - 8 * s == sub, 1.0, 0.0), a[s])
        w = tree([inv[k] * row_all(r, k) for k in range(8)])
        wr = [row_all(w, k) for k in range(8)]
        for t in range(NT):
            if t != s:
                acc = tree([lane_all(a[t], 8 * s + k) * wr[k] for k in range(8)])
                a[t] = jnp.where(inside, 0.0, a[t]) - acc
        a[s] = w
    return a


def split(x):
    hi = x.astype(BF16)
    return hi, (x - hi.astype(F32)).astype(BF16)


def dot(a, b):
    return jnp.dot(a, b, preferred_element_type=F32)


def dot3(a, b):
    return dot(a[0], b[0]) + (dot(a[0], b[1]) + dot(a[1], b[0]))


def dot3_t(a, b):
    t = lambda u, v: lax.dot_general(u, v, (((1,), (1,)), ((), ())), preferred_element_type=F32)
    return t(a[0], b[0]) + (t(a[0], b[1]) + t(a[1], b[0]))


NB = 6
HALF = 3
CUT = 1
SPAN = 1


def kernel(
    nz, nx, ny, tb, g_ref, out_ref, cb, rb, t11, fb, xs, dv, vb, lh, ll, xh, xl, yh, yl, zh, zl, vh, vl,
    rc, rm, rg, rt, rr, rf, s_scat, s_y, s_x, s_xf, s_m, s_g, s_t, s_r, sf,
):
    z, core, x, y = (lax.axis_index(a) for a in ("z", "core", "x", "y"))
    mate = 1 - core
    is0, is1 = core == 0, core == 1
    quarter = tb // nx
    top = z == 0
    root = is0 & top & (x == 0) & (y == 0)
    in_panel = (x == 0) & (y < 2)
    to_other = {"core": mate}
    pending = []

    def make(src, dst, send, recv, to):
        return pltpu.make_async_remote_copy(
            src_ref=src, dst_ref=dst, send_sem=send, recv_sem=recv, device_id=to, device_id_type=MESH
        )

    def put(cond, src, dst, send, recv, to):
        copy = make(src, dst, send, recv, to)
        pl.when(cond)(copy.start)
        pending.append((cond, copy))

    def arrived(cond, ref, recv):
        pl.when(cond)(make(ref, ref, s_t, recv, to_other).wait_recv)

    def near(i, n):
        return lax.rem(i + n, n)

    piece = quarter // CUT

    def rows(q, k):
        return pl.ds(pl.multiple_of(q * quarter + k * piece, 8), piece)

    for p in range(2):

        @pl.when((x == 0) & (y == p))
        def _():
            for h in range(2):
                cb[core, h, p] = g_ref[h].astype(F32)

    @pl.when(top)
    def _():
        rb[core] = g_ref[0].astype(F32)

    barrier = pltpu.get_barrier_semaphore()
    peers = [{"x": near(x + i, nx)} for i in range(1, nx)]
    for i in (-2, -1, 1, 2):
        peers += [{"y": near(y + i, ny)}, {"z": near(z + i, nz)}]
    peers += [to_other, {"y": y + 1 - 2 * lax.rem(y, 2), "core": mate}]
    for peer in peers:
        pl.semaphore_signal(barrier, inc=1, device_id=peer, device_id_type=MESH)
    pl.semaphore_wait(barrier, len(peers))

    def tree8(i, gate, last):
        hub = gate & ((i == 0) | (i == 2) | (i == 6))
        return [
            (hub, jnp.where(i == 0, 2, i - 1)),
            (hub, jnp.where(i == 0, 6, lax.rem(i + 1, 8))),
            (gate & last, 4),
        ]

    def r_rows(c):
        return pl.ds(c * quarter, quarter)

    def r_sends(c):
        ref, sem = rb.at[core, r_rows(c), :], rr.at[core, c]
        ways = [(cond, {"z": to}) for cond, to in tree8(z, z >= 0, (is0 & (z == 2)) | (is1 & (z == 6)))]
        ways += [(z >= 0, to_other)]
        return [(cond, make(ref, ref, s_r.at[c, n], sem, to)) for n, (cond, to) in enumerate(ways)]

    def r_relay(gate):
        @pl.when(gate)
        def _():
            for c in range(4):
                ref = rb.at[core, r_rows(c), :]
                pl.when(z > 0)(make(ref, ref, s_t, rr.at[core, c], to_other).wait_recv)
                for cond, copy in r_sends(c):
                    pl.when(cond)(copy.start)

    put(is1 & top & (x == 0) & (y == 1), cb.at[1, 0, 1], t11, s_t, rt, {"core": 0, "y": 0})
    for p in range(2):
        ref = cb.at[0, 1, p]
        put(is0 & top & (x == 0) & (y == p), ref, ref, s_g, rg, to_other)
    r_relay(top)

    busy = (z > 0) | is1

    def part(n):
        return jnp.where(top, 1 - n, core), jnp.where(top, 1, n)

    def scatter(n):
        r, h = part(n)
        for p in range(2):
            here = busy & (x == 0) & (y == p)
            if n:
                arrived(here & top, cb.at[0, 1, p], rg)
            for k in range(CUT):
                for q in (2, 1, 3):
                    ref = cb.at[r, h, p, rows(q, k), :]
                    put(here, ref, ref, s_scat.at[n, q - 1, k], rc.at[n, p, q, k], {"x": q})

    def to_mate(gate, n, p, q, k):
        if n:
            ref = cb.at[0, 1, p, rows(q, k), :]
            put(gate & top, ref, ref, s_m.at[p, q, k], rm.at[p, q, k], to_other)

    def spread(n):
        r, h = part(n)
        for k in range(CUT):
            for p in range(2):
                get = busy & ((x > 0) | (y != p))
                far = near(y - p, ny)
                ref, sem = cb.at[r, h, p, rows(x, k), :], rc.at[n, p, x, k]
                arrived(get, ref, sem)
                put(busy & (far < ny // 2), ref, ref, s_y.at[n, p, k, 0], sem, {"y": near(y + 1, ny)})
                back = busy & ((far == 0) | (far > ny // 2 + 1))
                put(back, ref, ref, s_y.at[n, p, k, 1], sem, {"y": near(y - 1, ny)})
                for i, side in enumerate((1, -1)):
                    to = near(x + side, nx)
                    put(busy & ((to > 0) | (y != p)), ref, ref, s_x.at[n, p, k, i], sem, {"x": to})
                to_mate(get, n, p, x, k)

    def gather(n):
        r, h = part(n)
        for k in range(CUT):
            for p in range(2):
                get = busy & ((x > 0) | (y != p))
                for side in (-1, 1):
                    q = near(x + side, nx)
                    ref, sem = cb.at[r, h, p, rows(q, k), :], rc.at[n, p, q, k]
                    arrived(get, ref, sem)
                    if side == (-1, 1)[p]:
                        to = near(x - side, nx)
                        put(busy & ((to > 0) | (y != p)), ref, ref, s_xf.at[n, p, k], sem, {"x": to})
                    to_mate(get, n, p, q, k)

    def gather_far(n):
        r, h = part(n)
        for k in range(CUT):
            for p in range(2):
                get = busy & ((x > 0) | (y != p))
                q = near(x + 2, nx)
                arrived(get, cb.at[r, h, p, rows(q, k), :], rc.at[n, p, q, k])
                to_mate(get, n, p, q, k)

    scatter(0)
    scatter(1)

    items = [(k, i) for k in range(NB) for i in range(k, NB, SPAN)]

    def blocks(k, i):
        return fb.at[k, i : min(i + SPAN, NB)]

    def item_sends(k, i):
        late = k >= NB - 2
        via = 2 if items.index((k, i)) % 2 else 6
        on_x = is0 & top & (y == 0)
        ways = [(on_x & (x == 0), {"x": 1}), (on_x & (x == 0), {"x": 3})]
        ways += [(on_x & (x == (0 if late else 1)), {"x": 2})]
        ways += [(c, {"y": to}) for c, to in tree8(y, is0 & top, y == via)]
        ways += [(c, {"z": to}) for c, to in tree8(z, is0, z == via)]
        ways += [(is0, to_other)]
        ref = blocks(k, i)
        return [(c, make(ref, ref, sf.at[k, i, n], rf.at[k, i], to)) for n, (c, to) in enumerate(ways)]

    def relay(gate, k, i):
        @pl.when(gate)
        def _():
            make(blocks(k, i), blocks(k, i), s_t, rf.at[k, i], to_other).wait_recv()
            for cond, copy in item_sends(k, i):
                pl.when(cond)(copy.start)

    @pl.when(root)
    def _():
        for c in range(4):
            make(rb.at[1, r_rows(c), :], rb.at[1, r_rows(c), :], s_t, rr.at[1, c], to_other).wait_recv()

        @pl.loop(0, NB)
        def _(j):
            for jj in range(NB):

                @pl.when(j == jj)
                def _():
                    lo = jj * B
                    if jj == HALF:
                        make(t11, t11, s_t, rt, to_other).wait_recv()
                    acc = 0.0
                    if jj:
                        acc = dot3_t((lh[lo:, :lo], ll[lo:, :lo]), (xh[lo : lo + B, :lo], xl[lo : lo + B, :lo]))
                    if jj < HALF:
                        a = jnp.concatenate([rb[0, lo:, lo : lo + B], rb[1, :, lo : lo + B]], axis=0)
                    else:
                        a = t11[lo - tb :, lo - tb : lo - tb + B]
                    xs[lo:, :] = a - acc

            o = pl.multiple_of(j * B, B)
            tiles = [xs[pl.ds(pl.multiple_of(o + 8 * i, 8), 8), :] for i in range(NT)]
            inv = inverse128(tiles)
            for i in range(NT):
                dv[8 * i : 8 * i + 8, :] = inv[i]
            for jj in range(NB):

                @pl.when(j == jj)
                def _():
                    lo = jj * B
                    fb[jj, jj] = dv[...]
                    if jj < NB - 1:
                        xc = split(xs[lo + B :, :])
                        w = dot3(xc, split(dv[...]))
                        wc = split(w)
                        xh[lo + B :, lo : lo + B], xl[lo + B :, lo : lo + B] = xc
                        lh[lo + B :, lo : lo + B], ll[lo + B :, lo : lo + B] = wc
                        for i in range(jj + 1, NB):
                            fb[jj, i] = w[(i - jj - 1) * B : (i - jj) * B, :]
                    for i in range(jj, NB, SPAN):
                        for cond, copy in item_sends(jj, i):
                            pl.when(cond)(copy.start)

    others = is0 & jnp.logical_not(root)
    hub = (z == 0) | (z == 2) | (z == 6)

    def step(k):
        for i in range(k, NB, SPAN):
            relay(others, k, i)

    spoke = (z == 2) | (z == 6)
    spread(0)
    r_relay(spoke)
    spread(1)
    step(0)
    gather(0)
    step(1)
    gather(1)
    step(2)
    step(3)
    step(4)
    r_relay(jnp.logical_not(spoke | top))
    relay(others & hub, *items[-1])

    for c in range(4):
        arrived(jnp.logical_not(root), rb.at[mate, r_rows(c), :], rr.at[mate, c])
    for k, i in items[:-1]:
        arrived(is1, blocks(k, i), rf.at[k, i])

    def unit(shape, shift):
        r = lax.broadcasted_iota(jnp.int32, shape, 0)
        return jnp.where(r - lax.broadcasted_iota(jnp.int32, shape, 1) == shift, 1.0, 0.0).astype(F32)

    def update(h, lo, hi, first):
        o = h * tb
        c = (vh[o : o + tb, lo:hi], vl[o : o + tb, lo:hi])
        w = (zh[lo:hi, :], zl[lo:hi, :])
        if first:
            keep = jnp.logical_not(in_panel | (top & (h == 0)))
            base = jnp.where(keep, g_ref[h].astype(F32), 0.0)
        else:
            base = out_ref[h]
        out_ref[h] = base - dot3(c, w)

    def solve(k):
        lo = k * B
        w = split(dot3(split(fb[k, k]), (yh[lo : lo + B, :], yl[lo : lo + B, :])))
        zh[lo : lo + B, :], zl[lo : lo + B, :] = w

    for k in range(NB):
        lo = k * B
        for j in range(k):
            lh[lo : lo + B, j * B : j * B + B], ll[lo : lo + B, j * B : j * B + B] = split(fb[j, k])
        p, off = k // HALF, k % HALF * B
        yk = jnp.where(in_panel, jnp.where(y == p, unit((B, tb), -off), 0.0), rb[p, off : off + B, :])
        if k:
            lk = (lh[lo : lo + B, :lo], ll[lo : lo + B, :lo])
            yk = yk - dot3(lk, (yh[:lo, :], yl[:lo, :]))
        yh[lo : lo + B, :], yl[lo : lo + B, :] = split(yk)
        if k < NB - 1:
            solve(k)

    def columns(h):
        o = h * tb
        for k in range(NB):
            lo = k * B
            p, off = k // HALF, k % HALF * B
            if h == 0:

                @pl.when(top)
                def _():
                    vb[...] = jnp.where(core == p, -unit((tb, B), off), 0.0)

                @pl.when(z > 0)
                def _():
                    vb[...] = cb[core, 0, p, :, off : off + B]

            vk = vb[...] if h == 0 else cb[core, h, p, :, off : off + B]
            if k:
                lk = (lh[lo : lo + B, :lo], ll[lo : lo + B, :lo])
                vk = vk - dot3_t((vh[o : o + tb, :lo], vl[o : o + tb, :lo]), lk)
            vh[o : o + tb, lo : lo + B], vl[o : o + tb, lo : lo + B] = split(vk)
        update(h, 0, (NB - 1) * B, True)

    gather_far(0)
    columns(0)
    gather_far(1)
    for p in range(2):
        for q in range(nx):
            for k in range(CUT):
                get = is0 & top & ((x > 0) | (y != p))
                arrived(get, cb.at[0, 1, p, rows(q, k), :], rm.at[p, q, k])
    columns(1)

    relay(others & jnp.logical_not(hub), *items[-1])
    arrived(is1, blocks(*items[-1]), rf.at[NB - 1, NB - 1])
    solve(NB - 1)
    for h in range(2):
        update(h, (NB - 1) * B, NB * B, False)

    for cond, copy in pending:
        pl.when(cond)(copy.wait_send)
    for copies in [r_sends(c) for c in range(4)] + [item_sends(k, i) for k, i in items]:
        for cond, copy in copies:
            pl.when(cond)(copy.wait_send)


def on_device(nz, nx, ny, gram):
    tb = gram.shape[2]
    block = gram.reshape(2, tb, tb)
    dma = pltpu.SemaphoreType.DMA
    n = 2 * tb
    wide = [pltpu.VMEM((n, n), BF16)]
    tall = [pltpu.VMEM((n, tb), BF16)]
    out = pl.pallas_call(
        functools.partial(kernel, nz, nx, ny, tb),
        out_shape=jax.ShapeDtypeStruct((2, tb, tb), F32),
        in_specs=[pl.BlockSpec(memory_space=pltpu.VMEM)],
        out_specs=pl.BlockSpec(memory_space=pltpu.VMEM),
        scratch_shapes=[
            pltpu.VMEM((2, 2, 2, tb, tb), F32),
            pltpu.VMEM((2, tb, tb), F32),
            pltpu.VMEM((tb, tb), F32),
            pltpu.VMEM((NB, NB, B, B), F32),
            pltpu.VMEM((n, B), F32),
            pltpu.VMEM((B, B), F32),
            pltpu.VMEM((tb, B), F32),
        ]
        + wide * 4 + tall * 4 + wide * 2
        + [
            dma((2, 2, nx, CUT)),
            dma((2, nx, CUT)),
            dma(()),
            dma(()),
            dma((2, 4)),
            dma((NB, NB)),
            dma((2, nx - 1, CUT)),
            dma((2, 2, CUT, 2)),
            dma((2, 2, CUT, 2)),
            dma((2, 2, CUT)),
            dma((2, nx, CUT)),
            dma(()),
            dma(()),
            dma((4, 4)),
            dma((NB, NB, 10)),
        ],
        compiler_params=pltpu.CompilerParams(
            collective_id=0, has_side_effects=True, vmem_limit_bytes=48 << 20
        ),
    )(block)
    return out.reshape(gram.shape)


def solution(mesh):
    shape = (8, 2, 4, 8)
    torus = Mesh(mesh.devices.reshape(shape), ("z", "core", "x", "y"))
    spec = P(None, ("z", "core"), None, None, ("x", "y"), None)
    return jax.shard_map(
        functools.partial(on_device, shape[0], shape[2], shape[3]),
        mesh=torus,
        in_specs=(spec,),
        out_specs=spec,
        check_vma=False,
    )
```

```python
import functools

import jax
import jax.numpy as jnp
from jax import lax
from jax.experimental import pallas as pl
from jax.experimental.pallas import tpu as pltpu
from jax.sharding import Mesh
from jax.sharding import PartitionSpec as P

F32, BF16 = jnp.float32, jnp.bfloat16
MESH = pl.DeviceIdType.MESH
B = 128
NT = B // 8


def row_all(x, k):
    return jnp.broadcast_to(x[k : k + 1, :], (8, 128))


def row_pick(x, k):
    return jnp.take_along_axis(x, jnp.full((8, 128), k, jnp.int32), axis=0)


def lane_all(x, j):
    return jnp.broadcast_to(x[:, j : j + 1], (8, 128))


def tree(xs):
    xs = list(xs)
    while len(xs) > 1:
        xs = [sum(xs[i : i + 2][1:], xs[i]) for i in range(0, len(xs), 2)]
    return xs[0]


def inverse8(cols, sub):
    cols = list(cols)
    pivot = row_pick(cols[0], 0)
    for k in range(8):
        q = 1.0 / pivot
        if k < 7:
            cross = row_pick(cols[k], k + 1) * row_pick(cols[k + 1], k)
            pivot = row_pick(cols[k + 1], k + 1) - cross * q
        own = sub == k
        cq = cols[k] * q
        new = []
        for j in range(8):
            if j == k:
                new.append(jnp.where(own, q, -cq))
            else:
                r = row_pick(cols[j], k)
                new.append(jnp.where(own, r * q, cols[j] - cq * r))
        cols = new
    return cols


def inverse128(tiles):
    lane = lax.broadcasted_iota(jnp.int32, (8, 128), 1)
    sub = lax.broadcasted_iota(jnp.int32, (8, 128), 0)
    a = list(tiles)
    for s in range(NT):
        inv = inverse8([lane_all(a[s], 8 * s + j) for j in range(8)], sub)
        inside = (lane >= 8 * s) & (lane < 8 * s + 8)
        r = jnp.where(inside, jnp.where(lane - 8 * s == sub, 1.0, 0.0), a[s])
        w = tree([inv[k] * row_all(r, k) for k in range(8)])
        wr = [row_all(w, k) for k in range(8)]
        for t in range(NT):
            if t != s:
                acc = tree([lane_all(a[t], 8 * s + k) * wr[k] for k in range(8)])
                a[t] = jnp.where(inside, 0.0, a[t]) - acc
        a[s] = w
    return a


def split(x):
    hi = x.astype(BF16)
    return hi, (x - hi.astype(F32)).astype(BF16)


def dot(a, b):
    return jnp.dot(a, b, preferred_element_type=F32)


def dot3(a, b):
    return dot(a[0], b[0]) + (dot(a[0], b[1]) + dot(a[1], b[0]))


def dot3_t(a, b):
    t = lambda u, v: lax.dot_general(u, v, (((1,), (1,)), ((), ())), preferred_element_type=F32)
    return t(a[0], b[0]) + (t(a[0], b[1]) + t(a[1], b[0]))


NB = 6
HALF = 3
CUT = 1
SPAN = 1


def kernel(
    nz, nx, ny, tb, g_ref, out_ref, cb, rb, t11, fb, xs, dv, vb, lh, ll, xh, xl, yh, yl, zh, zl, vh, vl,
    rc, rm, rg, rt, rr, rf, s_scat, s_y, s_x, s_xf, s_m, s_g, s_t, s_r, sf,
):
    z, core, x, y = (lax.axis_index(a) for a in ("z", "core", "x", "y"))
    mate = 1 - core
    is0, is1 = core == 0, core == 1
    quarter = tb // nx
    top = z == 0
    root = is0 & top & (x == 0) & (y == 0)
    in_panel = (x == 0) & (y < 2)
    to_other = {"core": mate}
    pending = []

    def make(src, dst, send, recv, to):
        return pltpu.make_async_remote_copy(
            src_ref=src, dst_ref=dst, send_sem=send, recv_sem=recv, device_id=to, device_id_type=MESH
        )

    def put(cond, src, dst, send, recv, to):
        copy = make(src, dst, send, recv, to)
        pl.when(cond)(copy.start)
        pending.append((cond, copy))

    def arrived(cond, ref, recv):
        pl.when(cond)(make(ref, ref, s_t, recv, to_other).wait_recv)

    def near(i, n):
        return lax.rem(i + n, n)

    piece = quarter // CUT

    def rows(q, k):
        return pl.ds(pl.multiple_of(q * quarter + k * piece, 8), piece)

    for p in range(2):

        @pl.when((x == 0) & (y == p))
        def _():
            for h in range(2):
                cb[core, h, p] = g_ref[h].astype(F32)

    @pl.when(top)
    def _():
        rb[core] = g_ref[0].astype(F32)

    barrier = pltpu.get_barrier_semaphore()
    peers = [{"x": near(x + i, nx)} for i in range(1, nx)]
    for i in (-2, -1, 1, 2):
        peers += [{"y": near(y + i, ny)}, {"z": near(z + i, nz)}]
    peers += [to_other, {"y": y + 1 - 2 * lax.rem(y, 2), "core": mate}]
    for peer in peers:
        pl.semaphore_signal(barrier, inc=1, device_id=peer, device_id_type=MESH)
    pl.semaphore_wait(barrier, len(peers))

    def tree8(i, gate, last):
        hub = gate & ((i == 0) | (i == 2) | (i == 6))
        return [
            (hub, jnp.where(i == 0, 2, i - 1)),
            (hub, jnp.where(i == 0, 6, lax.rem(i + 1, 8))),
            (gate & last, 4),
        ]

    def r_rows(c):
        return pl.ds(c * quarter, quarter)

    def r_sends(c):
        ref, sem = rb.at[core, r_rows(c), :], rr.at[core, c]
        ways = [(cond, {"z": to}) for cond, to in tree8(z, z >= 0, (is0 & (z == 2)) | (is1 & (z == 6)))]
        ways += [(z >= 0, to_other)]
        return [(cond, make(ref, ref, s_r.at[c, n], sem, to)) for n, (cond, to) in enumerate(ways)]

    def r_relay(gate):
        @pl.when(gate)
        def _():
            for c in range(4):
                ref = rb.at[core, r_rows(c), :]
                pl.when(z > 0)(make(ref, ref, s_t, rr.at[core, c], to_other).wait_recv)
                for cond, copy in r_sends(c):
                    pl.when(cond)(copy.start)

    put(is1 & top & (x == 0) & (y == 1), cb.at[1, 0, 1], t11, s_t, rt, {"core": 0, "y": 0})
    for p in range(2):
        ref = cb.at[0, 1, p]
        put(is0 & top & (x == 0) & (y == p), ref, ref, s_g, rg, to_other)
    r_relay(top)

    busy = (z > 0) | is1

    def part(n):
        return jnp.where(top, 1 - n, core), jnp.where(top, 1, n)

    def scatter(n):
        r, h = part(n)
        for p in range(2):
            here = busy & (x == 0) & (y == p)
            if n:
                arrived(here & top, cb.at[0, 1, p], rg)
            for k in range(CUT):
                for q in (2, 1, 3):
                    ref = cb.at[r, h, p, rows(q, k), :]
                    put(here, ref, ref, s_scat.at[n, q - 1, k], rc.at[n, p, q, k], {"x": q})

    def to_mate(gate, n, p, q, k):
        if n:
            ref = cb.at[0, 1, p, rows(q, k), :]
            put(gate & top, ref, ref, s_m.at[p, q, k], rm.at[p, q, k], to_other)

    def spread(n):
        r, h = part(n)
        for k in range(CUT):
            for p in range(2):
                get = busy & ((x > 0) | (y != p))
                far = near(y - p, ny)
                ref, sem = cb.at[r, h, p, rows(x, k), :], rc.at[n, p, x, k]
                arrived(get, ref, sem)
                put(busy & (far < ny // 2), ref, ref, s_y.at[n, p, k, 0], sem, {"y": near(y + 1, ny)})
                back = busy & ((far == 0) | (far > ny // 2 + 1))
                put(back, ref, ref, s_y.at[n, p, k, 1], sem, {"y": near(y - 1, ny)})
                for i, side in enumerate((1, -1)):
                    to = near(x + side, nx)
                    put(busy & ((to > 0) | (y != p)), ref, ref, s_x.at[n, p, k, i], sem, {"x": to})
                to_mate(get, n, p, x, k)

    def gather(n):
        r, h = part(n)
        for k in range(CUT):
            for p in range(2):
                get = busy & ((x > 0) | (y != p))
                for side in (-1, 1):
                    q = near(x + side, nx)
                    ref, sem = cb.at[r, h, p, rows(q, k), :], rc.at[n, p, q, k]
                    arrived(get, ref, sem)
                    if side == (-1, 1)[p]:
                        to = near(x - side, nx)
                        put(busy & ((to > 0) | (y != p)), ref, ref, s_xf.at[n, p, k], sem, {"x": to})
                    to_mate(get, n, p, q, k)

    def gather_far(n):
        r, h = part(n)
        for k in range(CUT):
            for p in range(2):
                get = busy & ((x > 0) | (y != p))
                q = near(x + 2, nx)
                arrived(get, cb.at[r, h, p, rows(q, k), :], rc.at[n, p, q, k])
                to_mate(get, n, p, q, k)

    scatter(0)
    scatter(1)

    items = [(k, i) for k in range(NB) for i in range(k, NB, SPAN)]

    def blocks(k, i):
        return fb.at[k, i : min(i + SPAN, NB)]

    def item_sends(k, i):
        late = k >= NB - 2
        on_x = is0 & top & (y == 0)
        ways = [(on_x & (x == 0), {"x": 1}), (on_x & (x == 0), {"x": 3})]
        ways += [(on_x & (x == (0 if late else 1)), {"x": 2})]
        ways += [(c, {"y": to}) for c, to in tree8(y, is0 & top, y == (2 if late else 3))]
        ways += [(c, {"z": to}) for c, to in tree8(z, is0, z == (2 if late else 3))]
        ways += [(is0, to_other)]
        ref = blocks(k, i)
        return [(c, make(ref, ref, sf.at[k, i, n], rf.at[k, i], to)) for n, (c, to) in enumerate(ways)]

    def relay(gate, k, i):
        @pl.when(gate)
        def _():
            make(blocks(k, i), blocks(k, i), s_t, rf.at[k, i], to_other).wait_recv()
            for cond, copy in item_sends(k, i):
                pl.when(cond)(copy.start)

    @pl.when(root)
    def _():
        for c in range(4):
            make(rb.at[1, r_rows(c), :], rb.at[1, r_rows(c), :], s_t, rr.at[1, c], to_other).wait_recv()

        @pl.loop(0, NB)
        def _(j):
            for jj in range(NB):

                @pl.when(j == jj)
                def _():
                    lo = jj * B
                    if jj == HALF:
                        make(t11, t11, s_t, rt, to_other).wait_recv()
                    acc = 0.0
                    if jj:
                        acc = dot3_t((lh[lo:, :lo], ll[lo:, :lo]), (xh[lo : lo + B, :lo], xl[lo : lo + B, :lo]))
                    if jj < HALF:
                        a = jnp.concatenate([rb[0, lo:, lo : lo + B], rb[1, :, lo : lo + B]], axis=0)
                    else:
                        a = t11[lo - tb :, lo - tb : lo - tb + B]
                    xs[lo:, :] = a - acc

            o = pl.multiple_of(j * B, B)
            tiles = [xs[pl.ds(pl.multiple_of(o + 8 * i, 8), 8), :] for i in range(NT)]
            inv = inverse128(tiles)
            for i in range(NT):
                dv[8 * i : 8 * i + 8, :] = inv[i]
            for jj in range(NB):

                @pl.when(j == jj)
                def _():
                    lo = jj * B
                    fb[jj, jj] = dv[...]
                    if jj < NB - 1:
                        xc = split(xs[lo + B :, :])
                        w = dot3(xc, split(dv[...]))
                        wc = split(w)
                        xh[lo + B :, lo : lo + B], xl[lo + B :, lo : lo + B] = xc
                        lh[lo + B :, lo : lo + B], ll[lo + B :, lo : lo + B] = wc
                        for i in range(jj + 1, NB):
                            fb[jj, i] = w[(i - jj - 1) * B : (i - jj) * B, :]
                    for i in range(jj, NB, SPAN):
                        for cond, copy in item_sends(jj, i):
                            pl.when(cond)(copy.start)

    others = is0 & jnp.logical_not(root)
    hub = (z == 0) | (z == 2) | (z == 6)

    def step(k):
        for i in range(k, NB, SPAN):
            relay(others, k, i)

    spoke = (z == 2) | (z == 6)
    distant = (y > 2) & (y < 7)
    r_relay(spoke & distant)
    spread(0)
    r_relay(spoke & jnp.logical_not(distant))
    spread(1)
    step(0)
    gather(0)
    step(1)
    gather(1)
    step(2)
    step(3)
    step(4)
    r_relay(jnp.logical_not(spoke | top))
    relay(others & hub, *items[-1])

    for c in range(4):
        arrived(jnp.logical_not(root), rb.at[mate, r_rows(c), :], rr.at[mate, c])
    for k, i in items[:-1]:
        arrived(is1, blocks(k, i), rf.at[k, i])

    def unit(shape, shift):
        r = lax.broadcasted_iota(jnp.int32, shape, 0)
        return jnp.where(r - lax.broadcasted_iota(jnp.int32, shape, 1) == shift, 1.0, 0.0).astype(F32)

    def update(h, lo, hi, first):
        o = h * tb
        c = (vh[o : o + tb, lo:hi], vl[o : o + tb, lo:hi])
        w = (zh[lo:hi, :], zl[lo:hi, :])
        if first:
            keep = jnp.logical_not(in_panel | (top & (h == 0)))
            base = jnp.where(keep, g_ref[h].astype(F32), 0.0)
        else:
            base = out_ref[h]
        out_ref[h] = base - dot3(c, w)

    def solve(k):
        lo = k * B
        w = split(dot3(split(fb[k, k]), (yh[lo : lo + B, :], yl[lo : lo + B, :])))
        zh[lo : lo + B, :], zl[lo : lo + B, :] = w

    for k in range(NB):
        lo = k * B
        for j in range(k):
            lh[lo : lo + B, j * B : j * B + B], ll[lo : lo + B, j * B : j * B + B] = split(fb[j, k])
        p, off = k // HALF, k % HALF * B
        yk = jnp.where(in_panel, jnp.where(y == p, unit((B, tb), -off), 0.0), rb[p, off : off + B, :])
        if k:
            lk = (lh[lo : lo + B, :lo], ll[lo : lo + B, :lo])
            yk = yk - dot3(lk, (yh[:lo, :], yl[:lo, :]))
        yh[lo : lo + B, :], yl[lo : lo + B, :] = split(yk)
        if k < NB - 1:
            solve(k)

    def columns(h):
        o = h * tb
        for k in range(NB):
            lo = k * B
            p, off = k // HALF, k % HALF * B
            if h == 0:

                @pl.when(top)
                def _():
                    vb[...] = jnp.where(core == p, -unit((tb, B), off), 0.0)

                @pl.when(z > 0)
                def _():
                    vb[...] = cb[core, 0, p, :, off : off + B]

            vk = vb[...] if h == 0 else cb[core, h, p, :, off : off + B]
            if k:
                lk = (lh[lo : lo + B, :lo], ll[lo : lo + B, :lo])
                vk = vk - dot3_t((vh[o : o + tb, :lo], vl[o : o + tb, :lo]), lk)
            vh[o : o + tb, lo : lo + B], vl[o : o + tb, lo : lo + B] = split(vk)
        update(h, 0, (NB - 1) * B, True)

    gather_far(0)
    columns(0)
    gather_far(1)
    for p in range(2):
        for q in range(nx):
            for k in range(CUT):
                get = is0 & top & ((x > 0) | (y != p))
                arrived(get, cb.at[0, 1, p, rows(q, k), :], rm.at[p, q, k])
    columns(1)

    relay(others & jnp.logical_not(hub), *items[-1])
    arrived(is1, blocks(*items[-1]), rf.at[NB - 1, NB - 1])
    solve(NB - 1)
    for h in range(2):
        update(h, (NB - 1) * B, NB * B, False)

    for cond, copy in pending:
        pl.when(cond)(copy.wait_send)
    for copies in [r_sends(c) for c in range(4)] + [item_sends(k, i) for k, i in items]:
        for cond, copy in copies:
            pl.when(cond)(copy.wait_send)


def on_device(nz, nx, ny, gram):
    tb = gram.shape[2]
    block = gram.reshape(2, tb, tb)
    dma = pltpu.SemaphoreType.DMA
    n = 2 * tb
    wide = [pltpu.VMEM((n, n), BF16)]
    tall = [pltpu.VMEM((n, tb), BF16)]
    out = pl.pallas_call(
        functools.partial(kernel, nz, nx, ny, tb),
        out_shape=jax.ShapeDtypeStruct((2, tb, tb), F32),
        in_specs=[pl.BlockSpec(memory_space=pltpu.VMEM)],
        out_specs=pl.BlockSpec(memory_space=pltpu.VMEM),
        scratch_shapes=[
            pltpu.VMEM((2, 2, 2, tb, tb), F32),
            pltpu.VMEM((2, tb, tb), F32),
            pltpu.VMEM((tb, tb), F32),
            pltpu.VMEM((NB, NB, B, B), F32),
            pltpu.VMEM((n, B), F32),
            pltpu.VMEM((B, B), F32),
            pltpu.VMEM((tb, B), F32),
        ]
        + wide * 4 + tall * 4 + wide * 2
        + [
            dma((2, 2, nx, CUT)),
            dma((2, nx, CUT)),
            dma(()),
            dma(()),
            dma((2, 4)),
            dma((NB, NB)),
            dma((2, nx - 1, CUT)),
            dma((2, 2, CUT, 2)),
            dma((2, 2, CUT, 2)),
            dma((2, 2, CUT)),
            dma((2, nx, CUT)),
            dma(()),
            dma(()),
            dma((4, 4)),
            dma((NB, NB, 10)),
        ],
        compiler_params=pltpu.CompilerParams(
            collective_id=0, has_side_effects=True, vmem_limit_bytes=48 << 20
        ),
    )(block)
    return out.reshape(gram.shape)


def solution(mesh):
    shape = (8, 2, 4, 8)
    torus = Mesh(mesh.devices.reshape(shape), ("z", "core", "x", "y"))
    spec = P(None, ("z", "core"), None, None, ("x", "y"), None)
    return jax.shard_map(
        functools.partial(on_device, shape[0], shape[2], shape[3]),
        mesh=torus,
        in_specs=(spec,),
        out_specs=spec,
        check_vma=False,
    )
```
